32 devices in a mesh: rows: 32 (over z, y, x, core).
Axes of the slice: x: 2, y: 2, z: 4, core: 2. Of those that a mesh axis runs over, the one named last changes fastest.
Arguments:
- left_factor: float32 [65536, 1024], P('rows'), may hold values from -6 to 6
- right_factor: float32 [65536, 1024], P('rows'), may hold values from -6 to 6
- tile_counts: int32 [32], P('rows'), may hold values from 1 to 4, as said below
- start_basis: float32 [1024, 256], replicated, may hold values from -6 to 6
Outputs:
- left_proj: float32 [65536, 256], P('rows')
- right_proj: float32 [65536, 256], P('rows')
The draws below stay inside these ranges and needn't reach their ends.
Inputs may be any that keep to these rules, and one draw needn't show every extreme that they name: `tile_counts`: each device's live slots are its first ones; some device has 4 live slots and some device has 1.
All inputs are finite; a program needn't handle non-finite values.
Results may differ from the reference program's by a relative error of at most 0.0002.
Values sent between devices are 32-bit elements; how exact they have to be, the bound alone decides.
A program may use at most 128 MiB of HBM per device.

```python
import jax
import jax.numpy as jnp
from jax import lax

STATES = 1024
RANK = 256
TILE = 512
SLOTS = 4
POWER = 2
ROWS_ALL = 65536
N_ROWS = 32


def draw_tile_counts(key, part):
    kinds = jax.random.randint(jax.random.fold_in(key, 11), (N_ROWS,), 0, 4)
    middle = max(1, SLOTS // 2)
    counts = jnp.where(kinds < 2, 1, jnp.where(kinds == 2, middle, SLOTS)).astype(jnp.int32)
    heavy = jax.random.randint(jax.random.fold_in(key, 12), (), 0, N_ROWS)
    offset = jax.random.randint(jax.random.fold_in(key, 13), (), 1, N_ROWS)
    light = (heavy + offset) % N_ROWS
    positions = jnp.arange(N_ROWS, dtype=jnp.int32)
    counts = jnp.where(positions == heavy, SLOTS, counts)
    counts = jnp.where(positions == light, 1, counts)
    return counts.astype(jnp.int32)


def steps_of(rng, shape, pieces, least, high):
    loudness = 1.0
    for position, blocks in pieces:
        heights = jax.random.uniform(jax.random.fold_in(jax.random.fold_in(rng, 6), position), (blocks,), jnp.float32, least / len(pieces), high / len(pieces))
        loudness = loudness * jnp.repeat(jnp.exp(heights), shape[position] // blocks).reshape((-1,) + (1,) * (len(shape) - 1 - position))
    return loudness


def normal_values(key, extent, scale, reach, cuts=(), kind=jnp.bfloat16):
    result = scale * jax.random.normal(key, extent, jnp.float32)
    if cuts:
        result = result * steps_of(key, extent, cuts, -0.22, 0.18)
    return jnp.clip(result, -reach, reach).astype(kind)


def setup_inputs(seed: int = 0) -> dict:
    seeds = jax.random.split(jax.random.key(seed), 5)
    return {
        "left_factor": normal_values(seeds[0], (ROWS_ALL, STATES), 1.0, 6.0, ((0, 32),), jnp.float32),
        "right_factor": normal_values(seeds[1], (ROWS_ALL, STATES), 1.0, 6.0, ((0, 32),), jnp.float32),
        "tile_counts": draw_tile_counts(jax.random.fold_in(seeds[4], 71), 0),
        "start_basis": normal_values(seeds[3], (STATES, RANK), 1.0, 6.0, (), jnp.float32),
    }


def product(left_side, right_side):
    return jnp.dot(left_side.astype(jnp.float32), right_side.astype(jnp.float32), precision=lax.Precision.HIGHEST, preferred_element_type=jnp.float32)

def transposed_product(left_side, right_side):
    return lax.dot_general(left_side.astype(jnp.float32), right_side.astype(jnp.float32), (((0,), (0,)), ((), ())), precision=lax.Precision.HIGHEST, preferred_element_type=jnp.float32)

def right_solve(factor, block):
    return jax.scipy.linalg.solve_triangular(factor, block.T, lower=True).T

def orthonormal(block):
    factor = jnp.linalg.cholesky(transposed_product(block, block))
    return right_solve(factor, block)

def reference(left_factor, right_factor, tile_counts, start_basis):
    devices = tile_counts.shape[0]
    slot_ids = jnp.arange(SLOTS, dtype=jnp.int32)
    live_slots = (slot_ids[None, :] < tile_counts[:, None]).astype(left_factor.dtype)
    row_mask = jnp.broadcast_to(live_slots[:, :, None], (devices, SLOTS, TILE)).reshape(-1, 1)
    gram_matrix = transposed_product(left_factor, right_factor * row_mask)
    current = start_basis
    for iteration in range(POWER):
        current = orthonormal(transposed_product(gram_matrix, product(gram_matrix, current)))
    image_cols = product(gram_matrix, current)
    square = transposed_product(image_cols, image_cols)
    factor = jnp.linalg.cholesky(square)
    left_map = right_solve(factor, image_cols)
    scaling = jnp.sqrt(jnp.trace(square) / RANK)
    right_map = right_solve(factor, current) * scaling
    left_proj = product(left_factor, left_map) * row_mask
    right_proj = product(right_factor, right_map) * row_mask
    return (left_proj, right_proj)
```

```python
import functools

import jax
import jax.numpy as jnp
from jax import lax
from jax.experimental import pallas as pl
from jax.experimental.pallas import tpu as pltpu
from jax.sharding import PartitionSpec as P

SLOTS = 4
POWER = 2
GROUP = 8
LANES = 128
MESH = pl.DeviceIdType.MESH
NN = (((1,), (0,)), ((), ()))
NT = (((1,), (1,)), ((), ()))


def split(value):
    high = value.astype(jnp.bfloat16)
    return high, (value - high.astype(jnp.float32)).astype(jnp.bfloat16)


def dot_pairs(left, right, dims):
    one = lambda a, b: lax.dot_general(a, b, dims, preferred_element_type=jnp.float32)
    return one(left[0], right[0]) + (one(left[0], right[1]) + one(left[1], right[0]))


def full_dot(left, right, dims=NN):
    return lax.dot_general(
        left, right, dims, precision=lax.Precision.HIGHEST, preferred_element_type=jnp.float32
    )


def grid_of(chips):
    bits = chips.bit_length() - 1
    inner = bits // 3
    middle = (bits - inner) // 2
    sizes = (2**inner, 2**middle, chips // 2 ** (inner + middle))
    return sizes


class Route:
    def __init__(self, chip, core, axes, half, flip):
        self.half = half
        self.sizes = [s for s, _ in axes]
        self.strides = [d for _, d in axes]
        self.digits = [lax.rem(chip // d, s) for s, d in axes]
        self.rows = [half]
        self.first = [0]
        for s, a in zip(self.sizes, self.digits):
            self.rows.append(self.rows[-1] // s)
            self.first.append(self.first[-1] + a * self.rows[-1])

def sum_kernel(chips, lags, part, high, low, *scratch):
    arrived, acc, total = scratch[:3]
    p_in, q_in = scratch[3:6], scratch[6:9]
    d2d, fwd = scratch[9:11]
    rs, ag = scratch[11:14], scratch[14:17]
    qrs, qag = scratch[17:20], scratch[20:23]
    me = lax.axis_index("rows")
    core = lax.rem(me, 2)
    chip = me // 2
    partner = me + 1 - 2 * core
    half = part.shape[0] // 2
    chunks = part.shape[1] // LANES
    kx, ky, kz = grid_of(chips)
    flat = kx == ky
    def pick(c, a, b):
        return a + c * (b - a) if flat else a
    def axes(c, z_first):
        plane = [(kx, pick(c, 1, kx)), (ky, pick(c, kx, 1))]
        line = (kz, kx * ky)
        return [line] + plane if z_first else plane + [line]
    mine = {z: Route(chip, core, axes(core, z), half, 0) for z in (False, True)}
    theirs = {z: Route(chip, core, axes(1 - core, z), half, 0) for z in (False, True)}

    def lanes(c):
        return pl.ds(c * LANES if isinstance(c, int) else pl.multiple_of(c * LANES, LANES), LANES)
    def rows(start, count, base=0):
        return pl.ds(pl.multiple_of(base + start, GROUP), count)
    def copy(src, dst, send, recv, device):
        return pltpu.make_async_remote_copy(src_ref=src, dst_ref=dst, send_sem=send, recv_sem=recv, device_id=(device,), device_id_type=MESH)

    last = chunks - 1
    my_base, its_base = core * half, (1 - core) * half

    def to_partner(c):
        return copy(part.at[rows(0, half, its_base), lanes(c)], arrived.at[c], d2d.at[0, c], d2d.at[1, c], partner)

    def peer(r, p, step):
        digit = lax.rem(r.digits[p] + step + r.sizes[p], r.sizes[p])
        return digit, 2 * (chip + (digit - r.digits[p]) * r.strides[p]) + core

    def rs_copy(z, p, c, u):
        r = mine[z]
        digit, device = peer(r, p, u)
        n = r.rows[p + 1]
        sems = (qrs if z else rs)[p]
        box = (q_in if z else p_in)[p]
        slot = 0 if z else c
        return copy(acc.at[c, rows(r.first[p] + digit * n, n)], box.at[slot, u - 1], sems.at[0, slot, u - 1], sems.at[1, slot, u - 1], device)

    def ag_copy(z, p, c, u, outgoing):
        r = mine[z]
        n = r.rows[p + 1]
        digit, device = peer(r, p, u if outgoing else -u)
        where = rows(r.first[p + 1] if outgoing else r.first[p] + digit * n, n, my_base)
        sems = (qag if z else ag)[p]
        slot = 0 if z else c
        return copy(total.at[c, where], total.at[c, where], sems.at[0, slot, u - 1], sems.at[1, slot, u - 1], device)

    def pieces(r, base):
        out = [rows(r.first[2], r.rows[2], base)]
        for p in (1, 0):
            for u in range(1, r.sizes[p]):
                digit = lax.rem(r.digits[p] - u + r.sizes[p], r.sizes[p])
                out.append(rows(r.first[p] + digit * r.rows[p + 1], r.rows[p + 1], base))
        return out

    def pass_on(z, c, i, outgoing):
        where = pieces(mine[z] if outgoing else theirs[z], my_base if outgoing else its_base)[i]
        return copy(total.at[c, where], total.at[c, where], fwd.at[0, c, i], fwd.at[1, c, i], partner)

    def put(c, where):
        pair = split(total[c, where, :])
        high[where, lanes(c)] = pair[0]
        low[where, lanes(c)] = pair[1]

    def rs_start(z, p, c):
        for u in range(1, mine[z].sizes[p]):
            rs_copy(z, p, c, u).start()

    def rs_finish(z, p, c):
        r = mine[z]
        for u in range(1, r.sizes[p]):
            rs_copy(z, p, c, u).wait_recv()
        where = rows(r.first[p + 1], r.rows[p + 1])
        box = (q_in if z else p_in)[p]
        slot = 0 if z else c
        value = acc[c, where, :]
        for u in range(1, r.sizes[p]):
            value += box[slot, u - 1]
        if p == 2:
            total[c, rows(r.first[3], r.rows[3], my_base), :] = value
        else:
            acc[c, where, :] = value

    def ag_start(z, p, c):
        for u in range(1, mine[z].sizes[p]):
            ag_copy(z, p, c, u, True).start()

    def ag_finish(z, p, c):
        for u in range(1, mine[z].sizes[p]):
            ag_copy(z, p, c, u, False).wait_recv()

    def event(kind, z, c):
        if kind == "D":
            to_partner(c).wait_recv()
            acc[c] = part[rows(0, half, my_base), lanes(c)] + arrived[c]
            rs_start(z, 0, c)
        elif kind in ("F1", "F2"):
            p = int(kind[1]) - 1
            rs_finish(z, p, c)
            rs_start(z, p + 1, c)
        elif kind == "F3":
            rs_finish(z, 2, c)
            ag_start(z, 2, c)
        elif kind == "A3":
            ag_finish(z, 2, c)
            ag_start(z, 1, c)
            pass_on(z, c, 0, True).start()
            put(c, pieces(mine[z], my_base)[0])
        elif kind == "A2":
            ag_finish(z, 1, c)
            ag_start(z, 0, c)
            for u in range(1, mine[z].sizes[1]):
                pass_on(z, c, u, True).start()
                put(c, pieces(mine[z], my_base)[u])
        elif kind == "A1":
            ag_finish(z, 0, c)
            for u in range(1, mine[z].sizes[0]):
                i = u + mine[z].sizes[1] - 1
                pass_on(z, c, i, True).start()
                put(c, pieces(mine[z], my_base)[i])
        else:
            for i, where in enumerate(pieces(theirs[z], its_base)):
                pass_on(z, c, i, False).wait_recv()
                put(c, where)

    def each(first, end, body):
        def step(u, carry):
            body(u)
            return carry
        lax.fori_loop(first, end, step, 0)

    barrier = pltpu.get_barrier_semaphore()
    devices = {}
    pl.semaphore_signal(barrier, inc=1, device_id=(partner,), device_id_type=MESH)
    count = 1
    for p in range(3):
        for u in range(1, mine[False].sizes[p]):
            pl.semaphore_signal(barrier, inc=1, device_id=(peer(mine[False], p, u)[1],), device_id_type=MESH)
            count += 1
    pl.semaphore_wait(barrier, count)

    to_partner(last).start()
    each(0, last, lambda c: to_partner(c).start())
    event("D", True, last)
    each(0, last, lambda c: event("D", False, c))

    q_lags = lags["Q"]
    end = 1 + max(last - 1 + max(v for k, v in lags.items() if k != "Q"), max(q_lags.values()))
    def step(t):
        for kind in ("F1", "F2", "F3", "A3", "A2", "A1", "W"):
            c = t - lags[kind]
            pl.when((c >= 0) & (c < last))(functools.partial(event, kind, False, c))
            pl.when(t == q_lags[kind])(functools.partial(event, kind, True, last))
    each(0, end, step)

    def drain(z, c):
        to_partner(c).wait_send()
        for p in range(3):
            for u in range(1, mine[z].sizes[p]):
                rs_copy(z, p, c, u).wait_send()
                ag_copy(z, p, c, u, True).wait_send()
        for i in range(len(pieces(mine[z], my_base))):
            pass_on(z, c, i, True).wait_send()
    each(0, last, lambda c: drain(False, c))
    drain(True, last)

LAGS = dict(F1=0, F2=1, F3=3, A3=5, A2=7, A1=9, W=10, Q=dict(F1=3, F2=4, F3=5, A3=7, A2=8, A1=12, W=13))

def sum_over_devices(part, devices, lags=LAGS):
    chips = devices // 2
    size, width = part.shape
    half = size // 2
    chunks = width // LANES
    kx, ky, kz = grid_of(chips)
    vmem = pl.BlockSpec(memory_space=pltpu.VMEM)
    dma = pltpu.SemaphoreType.DMA
    def boxes(order, slots):
        left, out = half, []
        for k in order:
            left //= k
            out.append(pltpu.VMEM((slots, k - 1, left, LANES), jnp.float32))
        return out
    def sems(order, slots):
        return [dma((2, slots, k - 1)) for k in order]
    p_order, q_order = (kx, ky, kz), (kz, kx, ky)
    scratch = [pltpu.VMEM((chunks, half, LANES), jnp.float32)] * 2 + [pltpu.VMEM((chunks, size, LANES), jnp.float32)]
    scratch += boxes(p_order, chunks - 1) + boxes(q_order, 1)
    fw = max(kx + ky - 1, kz + kx - 1)
    scratch += [dma((2, chunks)), dma((2, chunks, fw))]
    scratch += sems(p_order, chunks - 1) * 2 + sems(q_order, 1) * 2
    return pl.pallas_call(
        functools.partial(sum_kernel, chips, lags),
        out_shape=[jax.ShapeDtypeStruct(part.shape, jnp.bfloat16)] * 2,
        in_specs=[vmem],
        out_specs=[vmem, vmem],
        scratch_shapes=scratch,
        compiler_params=pltpu.CompilerParams(collective_id=0, has_side_effects=True, vmem_limit_bytes=48 * 2**20),
        name="sum_over_devices",
    )(part)


def inverse_factor(matrix):
    size = matrix.shape[0]
    groups = size // GROUP
    shape = (GROUP, size)
    row_ids = lax.broadcasted_iota(jnp.int32, shape, 0)
    lane_ids = lax.broadcasted_iota(jnp.int32, shape, 1)
    wide = lambda v: jnp.broadcast_to(v, shape)
    left = [matrix[GROUP * g : GROUP * (g + 1), :] for g in range(groups)]
    right = [jnp.where(lane_ids == row_ids + GROUP * g, 1.0, 0.0) for g in range(groups)]
    for g in range(groups):
        panel, beside = left[g], right[g]
        entry, factor, inverse, scale = {}, {}, {}, {}
        for j in range(GROUP):
            column = wide(panel[:, GROUP * g + j : GROUP * g + j + 1])
            for i in range(j, GROUP):
                entry[i, j] = wide(column[i : i + 1, :])
        for j in range(GROUP):
            scale[j] = lax.rsqrt(entry[j, j])
            for i in range(j + 1, GROUP):
                factor[i, j] = entry[i, j] * scale[j]
            for l in range(j + 1, GROUP):
                for i in range(l, GROUP):
                    entry[i, l] = entry[i, l] - factor[i, j] * factor[l, j]
        for j in range(GROUP):
            inverse[j, j] = scale[j]
            for i in range(j + 1, GROUP):
                acc = factor[i, j] * inverse[j, j]
                for l in range(j + 1, i):
                    acc = acc + factor[i, l] * inverse[l, j]
                inverse[i, j] = -acc * scale[i]
        new_panel, new_beside = jnp.zeros(shape, jnp.float32), jnp.zeros(shape, jnp.float32)
        for j in range(GROUP):
            column = jnp.zeros(shape, jnp.float32)
            for i in range(j, GROUP):
                column = jnp.where(row_ids == i, inverse[i, j], column)
            new_panel = new_panel + column * wide(panel[j : j + 1, :])
            new_beside = new_beside + column * wide(beside[j : j + 1, :])
        right[g] = new_beside
        if g + 1 < groups:
            turned = new_panel.T
            rows_of = [wide(new_panel[j : j + 1, :]) for j in range(GROUP)]
            beside_of = [wide(new_beside[j : j + 1, :]) for j in range(GROUP)]
            for r in range(g + 1, groups):
                tile = turned[GROUP * r : GROUP * (r + 1), :]
                for j in range(GROUP):
                    weight = wide(tile[:, j : j + 1])
                    left[r] = left[r] - weight * rows_of[j]
                    right[r] = right[r] - weight * beside_of[j]
    return jnp.concatenate(right, axis=0)


def chain_kernel(start, high, low, left_map, right_map, basis, image, square, inverse):
    rank = start.shape[0]
    cut = rank // 2
    basis[...] = start[...]
    inverse[...] = jnp.zeros_like(inverse)

    def turn(iteration, carry):
        gram = (high[...], low[...])
        image[...] = dot_pairs(split(basis[...]), gram, NT)

        @pl.when(iteration < POWER)
        def _():
            image[...] = dot_pairs(split(image[...]), (high[...], low[...]), NN)

        pair = split(image[...])
        square[...] = dot_pairs(pair, pair, NT)
        first = inverse_factor(square[:cut, :cut])
        across = full_dot(first, square[:cut, cut:])
        across_t = across.T
        second = inverse_factor(square[cut:, cut:] - full_dot(across_t, across))
        inverse[:cut, :cut] = first
        inverse[cut:, cut:] = second
        inverse[cut:, :cut] = -full_dot(second, full_dot(across_t, first))
        solved = split(inverse[...])

        @pl.when(iteration == POWER)
        def _():
            shape = square.shape
            diagonal = lax.broadcasted_iota(jnp.int32, shape, 0) == lax.broadcasted_iota(jnp.int32, shape, 1)
            trace = jnp.sum(jnp.where(diagonal, square[...], 0.0), keepdims=True)
            scaling = jnp.sqrt(trace / rank)
            right_map[...] = dot_pairs(solved, split(basis[...]), NN) * scaling
            left_map[...] = dot_pairs(solved, pair, NN)

        @pl.when(iteration < POWER)
        def _():
            basis[...] = dot_pairs(solved, pair, NN)

        return carry

    lax.fori_loop(0, POWER + 1, turn, 0)


def maps_of(start_rows, high, low):
    rank, states = start_rows.shape
    vmem = pl.BlockSpec(memory_space=pltpu.VMEM)
    small = pltpu.VMEM((rank, rank), jnp.float32)
    wide = pltpu.VMEM((rank, states), jnp.float32)
    return pl.pallas_call(
        chain_kernel,
        out_shape=[jax.ShapeDtypeStruct((rank, states), jnp.float32)] * 2,
        in_specs=[vmem] * 3,
        out_specs=[vmem] * 2,
        scratch_shapes=[wide, wide, small, small],
        compiler_params=pltpu.CompilerParams(vmem_limit_bytes=40 * 2**20),
        name="maps_of",
    )(start_rows, high, low)


def project(factor_rows, mapping, row_mask):
    rows = lax.dot_general(
        factor_rows, mapping, NT, precision=lax.Precision.HIGH, preferred_element_type=jnp.float32
    )
    return rows * row_mask


def local(devices, left_factor, right_factor, tile_counts, start_basis):
    tile_rows = left_factor.shape[0] // SLOTS
    live_count = tile_counts[0]
    slot_ids = lax.broadcasted_iota(jnp.int32, (SLOTS, 1, 1), 0)
    live_slots = (slot_ids < live_count).astype(jnp.float32)
    row_mask = jnp.broadcast_to(live_slots, (SLOTS, tile_rows, 1)).reshape(-1, 1)
    part = lax.dot_general(
        left_factor,
        right_factor * row_mask,
        (((0,), (0,)), ((), ())),
        precision=lax.Precision.HIGH,
        preferred_element_type=jnp.float32,
    )
    high, low = sum_over_devices(part, devices)
    left_map, right_map = maps_of(start_basis.T, high, low)
    return project(left_factor, left_map, row_mask), project(right_factor, right_map, row_mask)


def solution(mesh):
    return jax.shard_map(
        functools.partial(local, mesh.shape["rows"]),
        mesh=mesh,
        in_specs=(P("rows", None), P("rows", None), P("rows"), P()),
        out_specs=(P("rows", None), P("rows", None)),
        check_vma=False,
    )
```

```python
import functools

import jax
import jax.numpy as jnp
from jax import lax
from jax.experimental import pallas as pl
from jax.experimental.pallas import tpu as pltpu
from jax.sharding import PartitionSpec as P

SLOTS = 4
POWER = 2
GROUP = 8
LANES = 128
PANEL = 256
MESH = pl.DeviceIdType.MESH
NN = (((1,), (0,)), ((), ()))
NT = (((1,), (1,)), ((), ()))


def split(value):
    high = value.astype(jnp.bfloat16)
    return high, (value - high.astype(jnp.float32)).astype(jnp.bfloat16)


def dot_pairs(left, right, dims):
    one = lambda a, b: lax.dot_general(a, b, dims, preferred_element_type=jnp.float32)
    return one(left[0], right[0]) + (one(left[0], right[1]) + one(left[1], right[0]))


def full_dot(left, right, dims=NN):
    return lax.dot_general(
        left, right, dims, precision=lax.Precision.HIGHEST, preferred_element_type=jnp.float32
    )


def grid_of(chips):
    bits = chips.bit_length() - 1
    inner = bits // 3
    middle = (bits - inner) // 2
    sizes = (2**inner, 2**middle, chips // 2 ** (inner + middle))
    return sizes


class Route:
    def __init__(self, chip, core, axes, half, flip):
        self.half = half
        self.sizes = [s for s, _ in axes]
        self.strides = [d for _, d in axes]
        self.digits = [lax.rem(chip // d, s) for s, d in axes]
        self.rows = [half]
        self.first = [0]
        for s, a in zip(self.sizes, self.digits):
            self.rows.append(self.rows[-1] // s)
            self.first.append(self.first[-1] + a * self.rows[-1])

def sum_kernel(chips, lags, live, left, right, high, low, *scratch):
    lefts, rights, turned, masked, part, arrived, acc, total = scratch[:8]
    p_in, q_in = scratch[8:11], scratch[11:14]
    fetched, d2d, fwd = scratch[14:17]
    rs, ag = scratch[17:20], scratch[20:23]
    qrs, qag = scratch[23:26], scratch[26:29]
    me = lax.axis_index("rows")
    core = lax.rem(me, 2)
    chip = me // 2
    partner = me + 1 - 2 * core
    chunks, size = part.shape[:2]
    half = size // 2
    tile_rows = left.shape[0] // SLOTS
    blocks = size // PANEL
    kx, ky, kz = grid_of(chips)
    flat = kx == ky
    def pick(c, a, b):
        return a + c * (b - a) if flat else a
    def axes(c, z_first):
        plane = [(kx, pick(c, 1, kx)), (ky, pick(c, kx, 1))]
        line = (kz, kx * ky)
        return [line] + plane if z_first else plane + [line]
    mine = {z: Route(chip, core, axes(core, z), half, 0) for z in (False, True)}
    theirs = {z: Route(chip, core, axes(1 - core, z), half, 0) for z in (False, True)}

    def lanes(c):
        return pl.ds(c * LANES if isinstance(c, int) else pl.multiple_of(c * LANES, LANES), LANES)
    def rows(start, count, base=0):
        return pl.ds(pl.multiple_of(base + start, GROUP), count)
    def copy(src, dst, send, recv, device):
        return pltpu.make_async_remote_copy(src_ref=src, dst_ref=dst, send_sem=send, recv_sem=recv, device_id=(device,), device_id_type=MESH)

    my_base, its_base = core * half, (1 - core) * half

    def to_partner(c):
        return copy(part.at[c, rows(0, half, its_base)], arrived.at[c], d2d.at[0, c], d2d.at[1, c], partner)

    def peer(r, p, step):
        digit = lax.rem(r.digits[p] + step + r.sizes[p], r.sizes[p])
        return digit, 2 * (chip + (digit - r.digits[p]) * r.strides[p]) + core

    def rs_copy(z, p, c, u):
        r = mine[z]
        digit, device = peer(r, p, u)
        n = r.rows[p + 1]
        sems = (qrs if z else rs)[p]
        box = (q_in if z else p_in)[p]
        slot = 0 if z else c - 1
        return copy(acc.at[c, rows(r.first[p] + digit * n, n)], box.at[slot, u - 1], sems.at[0, slot, u - 1], sems.at[1, slot, u - 1], device)

    def ag_copy(z, p, c, u, outgoing):
        r = mine[z]
        n = r.rows[p + 1]
        digit, device = peer(r, p, u if outgoing else -u)
        where = rows(r.first[p + 1] if outgoing else r.first[p] + digit * n, n, my_base)
        sems = (qag if z else ag)[p]
        slot = 0 if z else c - 1
        return copy(total.at[c, where], total.at[c, where], sems.at[0, slot, u - 1], sems.at[1, slot, u - 1], device)

    def pieces(r, base):
        out = [rows(r.first[2], r.rows[2], base)]
        for p in (1, 0):
            for u in range(1, r.sizes[p]):
                digit = lax.rem(r.digits[p] - u + r.sizes[p], r.sizes[p])
                out.append(rows(r.first[p] + digit * r.rows[p + 1], r.rows[p + 1], base))
        return out

    def pass_on(z, c, i, outgoing):
        where = pieces(mine[z] if outgoing else theirs[z], my_base if outgoing else its_base)[i]
        return copy(total.at[c, where], total.at[c, where], fwd.at[0, c, i], fwd.at[1, c, i], partner)

    def put(c, where):
        pair = split(total[c, where, :])
        high[where, lanes(c)] = pair[0]
        low[where, lanes(c)] = pair[1]

    def rs_start(z, p, c):
        for u in range(1, mine[z].sizes[p]):
            rs_copy(z, p, c, u).start()

    def rs_finish(z, p, c):
        r = mine[z]
        for u in range(1, r.sizes[p]):
            rs_copy(z, p, c, u).wait_recv()
        where = rows(r.first[p + 1], r.rows[p + 1])
        box = (q_in if z else p_in)[p]
        slot = 0 if z else c - 1
        value = acc[c, where, :]
        for u in range(1, r.sizes[p]):
            value += box[slot, u - 1]
        if p == 2:
            total[c, rows(r.first[3], r.rows[3], my_base), :] = value
        else:
            acc[c, where, :] = value

    def ag_start(z, p, c):
        for u in range(1, mine[z].sizes[p]):
            ag_copy(z, p, c, u, True).start()

    def ag_finish(z, p, c):
        for u in range(1, mine[z].sizes[p]):
            ag_copy(z, p, c, u, False).wait_recv()

    def event(kind, z, c):
        if kind == "D":
            to_partner(c).wait_recv()
            acc[c] = part[c, rows(0, half, my_base), :] + arrived[c]
            rs_start(z, 0, c)
        elif kind in ("F1", "F2"):
            p = int(kind[1]) - 1
            rs_finish(z, p, c)
            rs_start(z, p + 1, c)
        elif kind == "F3":
            rs_finish(z, 2, c)
            ag_start(z, 2, c)
        elif kind == "A3":
            ag_finish(z, 2, c)
            ag_start(z, 1, c)
            pass_on(z, c, 0, True).start()
            put(c, pieces(mine[z], my_base)[0])
        elif kind == "A2":
            ag_finish(z, 1, c)
            ag_start(z, 0, c)
            for u in range(1, mine[z].sizes[1]):
                pass_on(z, c, u, True).start()
                put(c, pieces(mine[z], my_base)[u])
        elif kind == "A1":
            ag_finish(z, 0, c)
            for u in range(1, mine[z].sizes[0]):
                i = u + mine[z].sizes[1] - 1
                pass_on(z, c, i, True).start()
                put(c, pieces(mine[z], my_base)[i])
        else:
            for i, where in enumerate(pieces(theirs[z], its_base)):
                pass_on(z, c, i, False).wait_recv()
                put(c, where)

    def each(first, end, body):
        def step(u, carry):
            body(u)
            return carry
        lax.fori_loop(first, end, step, 0)

    barrier = pltpu.get_barrier_semaphore()
    pl.semaphore_signal(barrier, inc=1, device_id=(partner,), device_id_type=MESH)
    count = 1
    for p in range(3):
        for u in range(1, mine[False].sizes[p]):
            pl.semaphore_signal(barrier, inc=1, device_id=(peer(mine[False], p, u)[1],), device_id_type=MESH)
            count += 1
    pl.semaphore_wait(barrier, count)

    def fetch(s):
        where = pl.ds(pl.multiple_of(s * tile_rows, GROUP), tile_rows)
        slot = s % 2
        return (
            pltpu.make_async_copy(left.at[where], lefts.at[slot], fetched.at[0, s]),
            pltpu.make_async_copy(right.at[where], rights.at[slot], fetched.at[1, s]),
        )

    def fetch_start(s):
        for side in fetch(s):
            side.start()

    def product(n, m):
        one = lambda a, b: lax.dot_general(a, b, NN, preferred_element_type=jnp.float32)
        both = one(turned[m], masked[0, n])
        value = both[:PANEL] + (both[PANEL:] + one(turned[m, :PANEL], masked[1, n]))
        block = pl.ds(pl.multiple_of(m * PANEL, PANEL), PANEL)
        for h in range(PANEL // LANES):
            part[n * (PANEL // LANES) + h, block, :] = value[:, h * LANES : (h + 1) * LANES]

    def exchange(n):
        for h in range(PANEL // LANES):
            to_partner(n * (PANEL // LANES) + h).start()

    fetch_start(0)
    fetch_start(1)
    for s in range(SLOTS):
        for side in fetch(s):
            side.wait()
        mask = (s < live[0]).astype(jnp.float32)
        where = pl.ds(s * tile_rows, tile_rows)
        for m in range(blocks):
            lane = slice(m * PANEL, (m + 1) * PANEL)
            pair = split(rights[s % 2, :, lane] * mask)
            masked[0, m, where, :] = pair[0]
            masked[1, m, where, :] = pair[1]
            turn = split(lefts[s % 2, :, lane].T)
            turned[m, :PANEL, where] = turn[0]
            turned[m, PANEL:, where] = turn[1]
            if m == 0:
                first = pair
            value = dot_pairs(turn, first, NN)
            block = pl.ds(m * PANEL, PANEL)
            for h in range(PANEL // LANES):
                piece = value[:, h * LANES : (h + 1) * LANES]
                part[h, block, :] = piece if s == 0 else part[h, block, :] + piece
        if s + 2 < SLOTS:
            fetch_start(s + 2)
    exchange(0)

    q_lags = lags["Q"]
    stride = lags["stride"]
    kinds = ("F1", "F2", "F3", "A3", "A2", "A1", "W")
    steps = (blocks - 1) * blocks
    end = 1 + max(steps + lags["D"], lags["W"] + stride * (chunks - 1), q_lags["W"])

    def step(t):
        @pl.when(t < steps)
        def _():
            product(1 + t // blocks, lax.rem(t, blocks))

        @pl.when((t < steps) & (lax.rem(t, blocks) == blocks - 1))
        def _():
            exchange(1 + t // blocks)

        n = (t - lags["D"]) // blocks
        ready = (t >= lags["D"]) & (t <= steps + lags["D"]) & (lax.rem(t - lags["D"] + blocks, blocks) == 0)

        @pl.when(ready & (n == 0))
        def _():
            event("D", True, 0)
            for h in range(1, PANEL // LANES):
                event("D", False, h)

        @pl.when(ready & (n > 0))
        def _():
            for h in range(PANEL // LANES):
                event("D", False, n * (PANEL // LANES) + h)

        for kind in kinds:
            ahead = t - lags[kind]
            c = ahead // stride
            pl.when((ahead >= stride) & (c < chunks) & (lax.rem(ahead + stride, stride) == 0))(functools.partial(event, kind, False, c))
            pl.when(t == q_lags[kind])(functools.partial(event, kind, True, 0))

    each(0, end, step)

    def drain(z, c):
        to_partner(c).wait_send()
        for p in range(3):
            for u in range(1, mine[z].sizes[p]):
                rs_copy(z, p, c, u).wait_send()
                ag_copy(z, p, c, u, True).wait_send()
        for i in range(len(pieces(mine[z], my_base))):
            pass_on(z, c, i, True).wait_send()

    drain(True, 0)
    each(1, chunks, lambda c: drain(False, c))


LAGS = dict(stride=2, D=2, F1=7, F2=11, F3=15, A3=19, A2=23, A1=27, W=29, Q=dict(F1=12, F2=16, F3=19, A3=22, A2=25, A1=33, W=35))


def sum_over_devices(live, left, right, devices, lags=LAGS):
    chips = devices // 2
    rows, size = left.shape
    half = size // 2
    chunks = size // LANES
    blocks = size // PANEL
    tile_rows = rows // SLOTS
    kx, ky, kz = grid_of(chips)
    vmem = pl.BlockSpec(memory_space=pltpu.VMEM)
    smem = pl.BlockSpec(memory_space=pltpu.SMEM)
    hbm = pl.BlockSpec(memory_space=pl.ANY)
    dma = pltpu.SemaphoreType.DMA

    def boxes(order, slots):
        rest, out = half, []
        for k in order:
            rest //= k
            out.append(pltpu.VMEM((slots, k - 1, rest, LANES), jnp.float32))
        return out

    def sems(order, slots):
        return [dma((2, slots, k - 1)) for k in order]

    p_order, q_order = (kx, ky, kz), (kz, kx, ky)
    scratch = [pltpu.VMEM((2, tile_rows, size), jnp.float32)] * 2
    scratch += [pltpu.VMEM((blocks, 2 * PANEL, rows), jnp.bfloat16), pltpu.VMEM((2, blocks, rows, PANEL), jnp.bfloat16)]
    scratch += [pltpu.VMEM((chunks, size, LANES), jnp.float32)] + [pltpu.VMEM((chunks, half, LANES), jnp.float32)] * 2
    scratch += [pltpu.VMEM((chunks, size, LANES), jnp.float32)]
    scratch += boxes(p_order, chunks - 1) + boxes(q_order, 1)
    scratch += [dma((2, SLOTS)), dma((2, chunks)), dma((2, chunks, max(kx + ky - 1, kz + kx - 1)))]
    scratch += sems(p_order, chunks - 1) * 2 + sems(q_order, 1) * 2
    return pl.pallas_call(
        functools.partial(sum_kernel, chips, lags),
        out_shape=[jax.ShapeDtypeStruct((size, size), jnp.bfloat16)] * 2,
        in_specs=[smem, hbm, hbm],
        out_specs=[vmem, vmem],
        scratch_shapes=scratch,
        compiler_params=pltpu.CompilerParams(collective_id=0, has_side_effects=True, vmem_limit_bytes=48 * 2**20),
        name="gram_over_devices",
    )(live, left, right)


def inverse_factor(matrix, spread, beside):
    size = matrix.shape[0]
    groups = size // GROUP
    shape = (GROUP, size)
    row_ids = lax.broadcasted_iota(jnp.int32, shape, 0)
    lane_ids = lax.broadcasted_iota(jnp.int32, shape, 1)
    wide = lambda v: jnp.broadcast_to(v, shape)
    tiles = [matrix[GROUP * g : GROUP * (g + 1), :] for g in range(groups)]
    done = []
    for g in range(groups):
        first = GROUP * g
        columns = {r: [wide(tiles[r][:, first + j : first + j + 1]) for j in range(GROUP)] for r in range(g, groups)}
        for j in range(GROUP):
            spread[g, j] = columns[g][j]
        entry = {(i, j): spread[g, j, pl.ds(i, GROUP, stride=0), :] for j in range(GROUP) for i in range(j, GROUP)}
        here = (lane_ids >= first) & (lane_ids < first + GROUP)
        panel = jnp.where(here, jnp.where(lane_ids == row_ids + first, 1.0, 0.0), tiles[g])
        rows = [wide(panel[j : j + 1, :]) for j in range(GROUP)]
        factor, scale = {}, []
        for j in range(GROUP):
            scale.append(lax.rsqrt(entry[j, j]))
            rows[j] = rows[j] * scale[j]
            for i in range(j + 1, GROUP):
                factor[i, j] = entry[i, j] * scale[j]
            for l in range(j + 1, GROUP):
                for i in range(l, GROUP):
                    entry[i, l] = entry[i, l] - factor[i, j] * factor[l, j]
            for i in range(j + 1, GROUP):
                rows[i] = rows[i] - factor[i, j] * rows[j]
        beside(g)
        out = rows[0]
        for j in range(1, GROUP):
            out = jnp.where(row_ids == j, rows[j], out)
        done.append(jnp.where(lane_ids <= row_ids + first, out, 0.0))
        if g + 1 == groups:
            break
        solved = [rows[j] * scale[j] for j in range(GROUP)]
        rest = {r: jnp.where(here, 0.0, tiles[r]) for r in range(g + 1, groups)}
        for j in reversed(range(GROUP)):
            for l in range(j):
                solved[l] = solved[l] - (factor[j, l] * scale[l]) * solved[j]
            for r in range(g + 1, groups):
                rest[r] = rest[r] - columns[r][j] * solved[j]
        for r in rest:
            tiles[r] = rest[r]
    return jnp.concatenate(done, axis=0)


def maps_kernel(live, start, high, low, left, right, left_out, right_out, sides, products, now, image, after, square, inverse, earlier, spread, sems):
    rank = start.shape[1]
    cut = rank // 2
    rows = left.shape[0]
    tile_rows = rows // SLOTS
    fetch = [pltpu.make_async_copy(src, sides.at[i], sems.at[0, i]) for i, src in enumerate((left, right))]
    fetch[1].start()
    fetch[0].start()
    image[...] = dot_pairs(split(start[...].T), (high[...], low[...]), NT)
    now[...] = dot_pairs(split(image[...]), (high[...], low[...]), NN)
    inverse[...] = jnp.zeros_like(inverse)
    fetch[1].wait()
    fetch[0].wait()

    def turn(iteration, carry):
        side = jnp.where(iteration == POWER, 0, 1)
        pair = split(now[...])
        square[...] = dot_pairs(pair, pair, NT)

        def apply_gram(n):
            block = pl.ds(n * PANEL, PANEL)
            after[:, block] = dot_pairs(pair, (high[block, :], low[block, :]), NT)

        def apply_side(m):
            block = pl.ds(m * PANEL, PANEL)
            products[side, block, :] = dot_pairs(split(sides[side, block, :]), pair, NT)

        work = [functools.partial(apply_gram, n) for n in range(high.shape[0] // PANEL)]
        work += [functools.partial(apply_side, m) for m in range(rows // PANEL)]
        groups = cut // GROUP

        def beside(half, g):
            step = half * groups + g
            for job in work[step * len(work) // (2 * groups) : (step + 1) * len(work) // (2 * groups)]:
                job()

        first = inverse_factor(square[:cut, :cut], spread.at[0], functools.partial(beside, 0))
        across = full_dot(first, square[:cut, cut:])
        across_t = across.T
        second = inverse_factor(square[cut:, cut:] - full_dot(across_t, across), spread.at[1], functools.partial(beside, 1))
        inverse[:cut, :cut] = first
        inverse[cut:, cut:] = second
        inverse[cut:, :cut] = -full_dot(second, full_dot(across_t, first))

        @pl.when(iteration < POWER)
        def _():
            image[...] = dot_pairs(split(inverse[...]), split(after[...]), NN)

        @pl.when(iteration < POWER - 1)
        def _():
            now[...] = dot_pairs(split(image[...]), (high[...], low[...]), NN)

        @pl.when(iteration == POWER - 1)
        def _():
            now[...] = image[...]
            earlier[...] = inverse[...]

        return carry

    lax.fori_loop(0, POWER + 1, turn, 0)
    shape = square.shape
    diagonal = lax.broadcasted_iota(jnp.int32, shape, 0) == lax.broadcasted_iota(jnp.int32, shape, 1)
    trace = jnp.sum(jnp.where(diagonal, square[...], 0.0), keepdims=True)
    both = full_dot(inverse[...], earlier[...]) * jnp.sqrt(trace / rank)
    stores = []
    for side, (small, out) in enumerate(((inverse[...], left_out), (both, right_out))):
        small = split(small)
        for slot in range(SLOTS):
            block = pl.ds(slot * tile_rows, tile_rows)
            mask = (slot < live[0]).astype(jnp.float32)
            products[side, block, :] = dot_pairs(split(products[side, block, :]), small, NT) * mask
            stores.append(pltpu.make_async_copy(products.at[side, block], out.at[block], sems.at[1 + side, slot]))
            stores[-1].start()
    for store in stores:
        store.wait()


def project(left, right, live, start, high, low):
    states, rank = start.shape
    rows = left.shape[0]
    cut = rank // 2
    vmem = pl.BlockSpec(memory_space=pltpu.VMEM)
    smem = pl.BlockSpec(memory_space=pltpu.SMEM)
    hbm = pl.BlockSpec(memory_space=pl.ANY)
    small = pltpu.VMEM((rank, rank), jnp.float32)
    wide = pltpu.VMEM((rank, states), jnp.float32)
    return pl.pallas_call(
        maps_kernel,
        out_shape=[jax.ShapeDtypeStruct((rows, rank), jnp.float32)] * 2,
        in_specs=[smem, vmem, vmem, vmem, hbm, hbm],
        out_specs=[hbm, hbm],
        scratch_shapes=[
            pltpu.VMEM((2, rows, states), jnp.float32),
            pltpu.VMEM((2, rows, rank), jnp.float32),
            wide, wide, wide, small, small, small,
            pltpu.VMEM((2, cut // GROUP, GROUP, GROUP, cut), jnp.float32),
            pltpu.SemaphoreType.DMA((3, SLOTS)),
        ],
        compiler_params=pltpu.CompilerParams(vmem_limit_bytes=48 * 2**20),
        name="project",
    )(live, start, high, low, left, right)


def local(devices, left_factor, right_factor, tile_counts, start_basis):
    high, low = sum_over_devices(tile_counts, left_factor, right_factor, devices)
    return project(left_factor, right_factor, tile_counts, start_basis, high, low)


def solution(mesh):
    return jax.shard_map(
        functools.partial(local, mesh.shape["rows"]),
        mesh=mesh,
        in_specs=(P("rows", None), P("rows", None), P("rows"), P()),
        out_specs=(P("rows", None), P("rows", None)),
        check_vma=False,
    )
```

```python
import functools

import jax
import jax.numpy as jnp
from jax import lax
from jax.experimental import pallas as pl
from jax.experimental.pallas import tpu as pltpu
from jax.sharding import PartitionSpec as P

SLOTS = 4
POWER = 2
GROUP = 8
LANES = 128
PANEL = 256
MESH = pl.DeviceIdType.MESH
NN = (((1,), (0,)), ((), ()))
NT = (((1,), (1,)), ((), ()))


def split(value):
    high = value.astype(jnp.bfloat16)
    return high, (value - high.astype(jnp.float32)).astype(jnp.bfloat16)


def dot_pairs(left, right, dims):
    one = lambda a, b: lax.dot_general(a, b, dims, preferred_element_type=jnp.float32)
    return one(left[0], right[0]) + (one(left[0], right[1]) + one(left[1], right[0]))


def full_dot(left, right, dims=NN):
    return lax.dot_general(
        left, right, dims, precision=lax.Precision.HIGHEST, preferred_element_type=jnp.float32
    )


def grid_of(chips):
    bits = chips.bit_length() - 1
    inner = bits // 3
    middle = (bits - inner) // 2
    sizes = (2**inner, 2**middle, chips // 2 ** (inner + middle))
    return sizes


class Route:
    def __init__(self, chip, core, axes, half, flip):
        self.half = half
        self.sizes = [s for s, _ in axes]
        self.strides = [d for _, d in axes]
        self.digits = [lax.rem(chip // d, s) for s, d in axes]
        self.rows = [half]
        self.first = [0]
        for s, a in zip(self.sizes, self.digits):
            self.rows.append(self.rows[-1] // s)
            self.first.append(self.first[-1] + a * self.rows[-1])

def sum_kernel(chips, lags, live, left, right, high, low, *scratch):
    lefts, rights, turned, masked, part, arrived, acc, total = scratch[:8]
    p_in, q_in = scratch[8:11], scratch[11:14]
    fetched, d2d, fwd = scratch[14:17]
    rs, ag = scratch[17:20], scratch[20:23]
    qrs, qag = scratch[23:26], scratch[26:29]
    me = lax.axis_index("rows")
    core = lax.rem(me, 2)
    chip = me // 2
    partner = me + 1 - 2 * core
    chunks, size = part.shape[:2]
    half = size // 2
    tile_rows = left.shape[0] // SLOTS
    blocks = size // PANEL
    kx, ky, kz = grid_of(chips)
    flat = kx == ky
    def pick(c, a, b):
        return a + c * (b - a) if flat else a
    def axes(c, z_first):
        plane = [(kx, pick(c, 1, kx)), (ky, pick(c, kx, 1))]
        line = (kz, kx * ky)
        return [line] + plane if z_first else plane + [line]
    mine = {z: Route(chip, core, axes(core, z), half, 0) for z in (False, True)}
    theirs = {z: Route(chip, core, axes(1 - core, z), half, 0) for z in (False, True)}

    def lanes(c):
        return pl.ds(c * LANES if isinstance(c, int) else pl.multiple_of(c * LANES, LANES), LANES)
    def rows(start, count, base=0):
        return pl.ds(pl.multiple_of(base + start, GROUP), count)
    def copy(src, dst, send, recv, device):
        return pltpu.make_async_remote_copy(src_ref=src, dst_ref=dst, send_sem=send, recv_sem=recv, device_id=(device,), device_id_type=MESH)

    my_base, its_base = core * half, (1 - core) * half

    def to_partner(c):
        return copy(part.at[c, rows(0, half, its_base)], arrived.at[c], d2d.at[0, c], d2d.at[1, c], partner)

    def peer(r, p, step):
        digit = lax.rem(r.digits[p] + step + r.sizes[p], r.sizes[p])
        return digit, 2 * (chip + (digit - r.digits[p]) * r.strides[p]) + core

    def rs_copy(z, p, c, u):
        r = mine[z]
        digit, device = peer(r, p, u)
        n = r.rows[p + 1]
        sems = (qrs if z else rs)[p]
        box = (q_in if z else p_in)[p]
        slot = 0 if z else c - 1
        return copy(acc.at[c, rows(r.first[p] + digit * n, n)], box.at[slot, u - 1], sems.at[0, slot, u - 1], sems.at[1, slot, u - 1], device)

    def ag_copy(z, p, c, u, outgoing):
        r = mine[z]
        n = r.rows[p + 1]
        digit, device = peer(r, p, u if outgoing else -u)
        where = rows(r.first[p + 1] if outgoing else r.first[p] + digit * n, n, my_base)
        sems = (qag if z else ag)[p]
        slot = 0 if z else c - 1
        return copy(total.at[c, where], total.at[c, where], sems.at[0, slot, u - 1], sems.at[1, slot, u - 1], device)

    def pieces(r, base):
        out = [rows(r.first[2], r.rows[2], base)]
        for p in (1, 0):
            for u in range(1, r.sizes[p]):
                digit = lax.rem(r.digits[p] - u + r.sizes[p], r.sizes[p])
                out.append(rows(r.first[p] + digit * r.rows[p + 1], r.rows[p + 1], base))
        return out

    def pass_on(z, c, i, outgoing):
        where = pieces(mine[z] if outgoing else theirs[z], my_base if outgoing else its_base)[i]
        return copy(total.at[c, where], total.at[c, where], fwd.at[0, c, i], fwd.at[1, c, i], partner)

    def put(c, where):
        pair = split(total[c, where, :])
        high[where, lanes(c)] = pair[0]
        low[where, lanes(c)] = pair[1]

    def rs_start(z, p, c):
        for u in range(1, mine[z].sizes[p]):
            rs_copy(z, p, c, u).start()

    def rs_finish(z, p, c):
        r = mine[z]
        for u in range(1, r.sizes[p]):
            rs_copy(z, p, c, u).wait_recv()
        where = rows(r.first[p + 1], r.rows[p + 1])
        box = (q_in if z else p_in)[p]
        slot = 0 if z else c - 1
        value = acc[c, where, :]
        for u in range(1, r.sizes[p]):
            value += box[slot, u - 1]
        if p == 2:
            total[c, rows(r.first[3], r.rows[3], my_base), :] = value
        else:
            acc[c, where, :] = value

    def ag_start(z, p, c):
        for u in range(1, mine[z].sizes[p]):
            ag_copy(z, p, c, u, True).start()

    def ag_finish(z, p, c):
        for u in range(1, mine[z].sizes[p]):
            ag_copy(z, p, c, u, False).wait_recv()

    def event(kind, z, c):
        if kind == "D":
            to_partner(c).wait_recv()
            acc[c] = part[c, rows(0, half, my_base), :] + arrived[c]
            rs_start(z, 0, c)
        elif kind in ("F1", "F2"):
            p = int(kind[1]) - 1
            rs_finish(z, p, c)
            rs_start(z, p + 1, c)
        elif kind == "F3":
            rs_finish(z, 2, c)
            ag_start(z, 2, c)
        elif kind == "A3":
            ag_finish(z, 2, c)
            ag_start(z, 1, c)
            pass_on(z, c, 0, True).start()
            put(c, pieces(mine[z], my_base)[0])
        elif kind == "A2":
            ag_finish(z, 1, c)
            ag_start(z, 0, c)
            for u in range(1, mine[z].sizes[1]):
                pass_on(z, c, u, True).start()
                put(c, pieces(mine[z], my_base)[u])
        elif kind == "A1":
            ag_finish(z, 0, c)
            for u in range(1, mine[z].sizes[0]):
                i = u + mine[z].sizes[1] - 1
                pass_on(z, c, i, True).start()
                put(c, pieces(mine[z], my_base)[i])
        else:
            for i, where in enumerate(pieces(theirs[z], its_base)):
                pass_on(z, c, i, False).wait_recv()
                put(c, where)

    def each(first, end, body):
        def step(u, carry):
            body(u)
            return carry
        lax.fori_loop(first, end, step, 0)

    barrier = pltpu.get_barrier_semaphore()
    pl.semaphore_signal(barrier, inc=1, device_id=(partner,), device_id_type=MESH)
    count = 1
    for p in range(3):
        for u in range(1, mine[False].sizes[p]):
            pl.semaphore_signal(barrier, inc=1, device_id=(peer(mine[False], p, u)[1],), device_id_type=MESH)
            count += 1
    pl.semaphore_wait(barrier, count)

    def fetch(s):
        where = pl.ds(pl.multiple_of(s * tile_rows, GROUP), tile_rows)
        slot = s % 2
        return (
            pltpu.make_async_copy(left.at[where], lefts.at[slot], fetched.at[0, s]),
            pltpu.make_async_copy(right.at[where], rights.at[slot], fetched.at[1, s]),
        )

    def fetch_start(s):
        for side in fetch(s):
            side.start()

    def product(n, m):
        one = lambda a, b: lax.dot_general(a, b, NN, preferred_element_type=jnp.float32)
        both = one(turned[m], masked[0, n])
        value = both[:PANEL] + (both[PANEL:] + one(turned[m, :PANEL], masked[1, n]))
        block = pl.ds(pl.multiple_of(m * PANEL, PANEL), PANEL)
        for h in range(PANEL // LANES):
            part[n * (PANEL // LANES) + h, block, :] = value[:, h * LANES : (h + 1) * LANES]

    def exchange(n):
        for h in range(PANEL // LANES):
            to_partner(n * (PANEL // LANES) + h).start()

    fetch_start(0)
    fetch_start(1)
    for s in range(SLOTS):
        for side in fetch(s):
            side.wait()
        mask = (s < live[0]).astype(jnp.float32)
        where = pl.ds(s * tile_rows, tile_rows)
        for m in range(blocks):
            lane = slice(m * PANEL, (m + 1) * PANEL)
            pair = split(rights[s % 2, :, lane] * mask)
            masked[0, m, where, :] = pair[0]
            masked[1, m, where, :] = pair[1]
            turn = split(lefts[s % 2, :, lane].T)
            turned[m, :PANEL, where] = turn[0]
            turned[m, PANEL:, where] = turn[1]
            if m == 0:
                first = pair
            value = dot_pairs(turn, first, NN)
            block = pl.ds(m * PANEL, PANEL)
            for h in range(PANEL // LANES):
                piece = value[:, h * LANES : (h + 1) * LANES]
                part[h, block, :] = piece if s == 0 else part[h, block, :] + piece
        if s + 2 < SLOTS:
            fetch_start(s + 2)
    exchange(0)

    q_lags = lags["Q"]
    stride = lags["stride"]
    kinds = ("F1", "F2", "F3", "A3", "A2", "A1", "W")
    steps = (blocks - 1) * blocks
    end = 1 + max(steps + lags["D"], lags["W"] + stride * (chunks - 1), q_lags["W"])

    def step(t):
        @pl.when(t < steps)
        def _():
            product(1 + t // blocks, lax.rem(t, blocks))

        @pl.when((t < steps) & (lax.rem(t, blocks) == blocks - 1))
        def _():
            exchange(1 + t // blocks)

        n = (t - lags["D"]) // blocks
        ready = (t >= lags["D"]) & (t <= steps + lags["D"]) & (lax.rem(t - lags["D"] + blocks, blocks) == 0)

        @pl.when(ready & (n == 0))
        def _():
            event("D", True, 0)
            for h in range(1, PANEL // LANES):
                event("D", False, h)

        @pl.when(ready & (n > 0))
        def _():
            for h in range(PANEL // LANES):
                event("D", False, n * (PANEL // LANES) + h)

        for kind in kinds:
            ahead = t - lags[kind]
            c = ahead // stride
            pl.when((ahead >= stride) & (c < chunks) & (lax.rem(ahead + stride, stride) == 0))(functools.partial(event, kind, False, c))
            pl.when(t == q_lags[kind])(functools.partial(event, kind, True, 0))

    each(0, end, step)

    def drain(z, c):
        to_partner(c).wait_send()
        for p in range(3):
            for u in range(1, mine[z].sizes[p]):
                rs_copy(z, p, c, u).wait_send()
                ag_copy(z, p, c, u, True).wait_send()
        for i in range(len(pieces(mine[z], my_base))):
            pass_on(z, c, i, True).wait_send()

    drain(True, 0)
    each(1, chunks, lambda c: drain(False, c))


LAGS = dict(stride=2, D=2, F1=7, F2=11, F3=15, A3=19, A2=23, A1=27, W=29, Q=dict(F1=12, F2=16, F3=19, A3=22, A2=25, A1=33, W=35))


def sum_over_devices(live, left, right, devices, lags=LAGS):
    chips = devices // 2
    rows, size = left.shape
    half = size // 2
    chunks = size // LANES
    blocks = size // PANEL
    tile_rows = rows // SLOTS
    kx, ky, kz = grid_of(chips)
    vmem = pl.BlockSpec(memory_space=pltpu.VMEM)
    smem = pl.BlockSpec(memory_space=pltpu.SMEM)
    hbm = pl.BlockSpec(memory_space=pl.ANY)
    dma = pltpu.SemaphoreType.DMA

    def boxes(order, slots):
        rest, out = half, []
        for k in order:
            rest //= k
            out.append(pltpu.VMEM((slots, k - 1, rest, LANES), jnp.float32))
        return out

    def sems(order, slots):
        return [dma((2, slots, k - 1)) for k in order]

    p_order, q_order = (kx, ky, kz), (kz, kx, ky)
    scratch = [pltpu.VMEM((2, tile_rows, size), jnp.float32)] * 2
    scratch += [pltpu.VMEM((blocks, 2 * PANEL, rows), jnp.bfloat16), pltpu.VMEM((2, blocks, rows, PANEL), jnp.bfloat16)]
    scratch += [pltpu.VMEM((chunks, size, LANES), jnp.float32)] + [pltpu.VMEM((chunks, half, LANES), jnp.float32)] * 2
    scratch += [pltpu.VMEM((chunks, size, LANES), jnp.float32)]
    scratch += boxes(p_order, chunks - 1) + boxes(q_order, 1)
    scratch += [dma((2, SLOTS)), dma((2, chunks)), dma((2, chunks, max(kx + ky - 1, kz + kx - 1)))]
    scratch += sems(p_order, chunks - 1) * 2 + sems(q_order, 1) * 2
    return pl.pallas_call(
        functools.partial(sum_kernel, chips, lags),
        out_shape=[jax.ShapeDtypeStruct((size, size), jnp.bfloat16)] * 2,
        in_specs=[smem, hbm, hbm],
        out_specs=[vmem, vmem],
        scratch_shapes=scratch,
        compiler_params=pltpu.CompilerParams(collective_id=0, has_side_effects=True, vmem_limit_bytes=48 * 2**20),
        name="gram_over_devices",
    )(live, left, right)


def inverse_factor(matrix, spread, beside):
    size = matrix.shape[0]
    groups = size // GROUP
    shape = (GROUP, size)
    row_ids = lax.broadcasted_iota(jnp.int32, shape, 0)
    lane_ids = lax.broadcasted_iota(jnp.int32, shape, 1)
    wide = lambda v: jnp.broadcast_to(v, shape)
    tiles = [matrix[GROUP * g : GROUP * (g + 1), :] for g in range(groups)]
    done = []
    for g in range(groups):
        first = GROUP * g
        columns = {r: [wide(tiles[r][:, first + j : first + j + 1]) for j in range(GROUP)] for r in range(g, groups)}
        for j in range(GROUP):
            spread[g, j] = columns[g][j]
        entry = {(i, j): spread[g, j, pl.ds(i, GROUP, stride=0), :] for j in range(GROUP) for i in range(j, GROUP)}
        here = (lane_ids >= first) & (lane_ids < first + GROUP)
        panel = jnp.where(here, jnp.where(lane_ids == row_ids + first, 1.0, 0.0), tiles[g])
        rows = [wide(panel[j : j + 1, :]) for j in range(GROUP)]
        factor, scale = {}, []
        for j in range(GROUP):
            scale.append(lax.rsqrt(entry[j, j]))
            rows[j] = rows[j] * scale[j]
            for i in range(j + 1, GROUP):
                factor[i, j] = entry[i, j] * scale[j]
            for l in range(j + 1, GROUP):
                for i in range(l, GROUP):
                    entry[i, l] = entry[i, l] - factor[i, j] * factor[l, j]
            for i in range(j + 1, GROUP):
                rows[i] = rows[i] - factor[i, j] * rows[j]
        beside(g)
        out = rows[0]
        for j in range(1, GROUP):
            out = jnp.where(row_ids == j, rows[j], out)
        done.append(jnp.where(lane_ids <= row_ids + first, out, 0.0))
        if g + 1 == groups:
            break
        solved = [rows[j] * scale[j] for j in range(GROUP)]
        rest = {r: jnp.where(here, 0.0, tiles[r]) for r in range(g + 1, groups)}
        for j in reversed(range(GROUP)):
            for l in range(j):
                solved[l] = solved[l] - (factor[j, l] * scale[l]) * solved[j]
            for r in range(g + 1, groups):
                rest[r] = rest[r] - columns[r][j] * solved[j]
        for r in rest:
            tiles[r] = rest[r]
    return jnp.concatenate(done, axis=0)


def maps_kernel(live, start, high, low, left, right, left_out, right_out, sides, products, now, image, after, square, inverse, earlier, spread, sems):
    rank = start.shape[1]
    cut = rank // 2
    rows = left.shape[0]
    tile_rows = rows // SLOTS
    fetch = [pltpu.make_async_copy(src, sides.at[i], sems.at[0, i]) for i, src in enumerate((left, right))]
    fetch[1].start()
    fetch[0].start()
    image[...] = dot_pairs(split(start[...].T), (high[...], low[...]), NT)
    now[...] = dot_pairs(split(image[...]), (high[...], low[...]), NN)
    inverse[...] = jnp.zeros_like(inverse)
    fetch[1].wait()

    def turn(iteration, carry):
        side = jnp.where(iteration == POWER, 0, 1)

        @pl.when(iteration == POWER)
        def _():
            fetch[0].wait()

        pair = split(now[...])
        square[...] = dot_pairs(pair, pair, NT)

        def apply_gram(n):
            block = pl.ds(n * PANEL, PANEL)
            after[:, block] = dot_pairs(pair, (high[block, :], low[block, :]), NT)

        def apply_side(m):
            block = pl.ds(m * PANEL, PANEL)
            products[side, block, :] = dot_pairs(split(sides[side, block, :]), pair, NT)

        work = [functools.partial(apply_gram, n) for n in range(high.shape[0] // PANEL)]
        work += [functools.partial(apply_side, m) for m in range(rows // PANEL)]
        groups = cut // GROUP

        def beside(half, g):
            step = half * groups + g
            for job in work[step * len(work) // (2 * groups) : (step + 1) * len(work) // (2 * groups)]:
                job()

        first = inverse_factor(square[:cut, :cut], spread.at[0], functools.partial(beside, 0))
        across = full_dot(first, square[:cut, cut:])
        across_t = across.T
        second = inverse_factor(square[cut:, cut:] - full_dot(across_t, across), spread.at[1], functools.partial(beside, 1))
        inverse[:cut, :cut] = first
        inverse[cut:, cut:] = second
        inverse[cut:, :cut] = -full_dot(second, full_dot(across_t, first))

        @pl.when(iteration < POWER)
        def _():
            image[...] = dot_pairs(split(inverse[...]), split(after[...]), NN)

        @pl.when(iteration < POWER - 1)
        def _():
            now[...] = dot_pairs(split(image[...]), (high[...], low[...]), NN)

        @pl.when(iteration == POWER - 1)
        def _():
            now[...] = image[...]
            earlier[...] = inverse[...]

        return carry

    lax.fori_loop(0, POWER + 1, turn, 0)
    shape = square.shape
    diagonal = lax.broadcasted_iota(jnp.int32, shape, 0) == lax.broadcasted_iota(jnp.int32, shape, 1)
    trace = jnp.sum(jnp.where(diagonal, square[...], 0.0), keepdims=True)
    both = full_dot(inverse[...], earlier[...]) * jnp.sqrt(trace / rank)
    stores = []
    for side, (small, out) in enumerate(((inverse[...], left_out), (both, right_out))):
        small = split(small)
        for slot in range(SLOTS):
            block = pl.ds(slot * tile_rows, tile_rows)
            mask = (slot < live[0]).astype(jnp.float32)
            products[side, block, :] = dot_pairs(split(products[side, block, :]), small, NT) * mask
            stores.append(pltpu.make_async_copy(products.at[side, block], out.at[block], sems.at[1 + side, slot]))
            stores[-1].start()
    for store in stores:
        store.wait()


def project(left, right, live, start, high, low):
    states, rank = start.shape
    rows = left.shape[0]
    cut = rank // 2
    vmem = pl.BlockSpec(memory_space=pltpu.VMEM)
    smem = pl.BlockSpec(memory_space=pltpu.SMEM)
    hbm = pl.BlockSpec(memory_space=pl.ANY)
    small = pltpu.VMEM((rank, rank), jnp.float32)
    wide = pltpu.VMEM((rank, states), jnp.float32)
    return pl.pallas_call(
        maps_kernel,
        out_shape=[jax.ShapeDtypeStruct((rows, rank), jnp.float32)] * 2,
        in_specs=[smem, vmem, vmem, vmem, hbm, hbm],
        out_specs=[hbm, hbm],
        scratch_shapes=[
            pltpu.VMEM((2, rows, states), jnp.float32),
            pltpu.VMEM((2, rows, rank), jnp.float32),
            wide, wide, wide, small, small, small,
            pltpu.VMEM((2, cut // GROUP, GROUP, GROUP, cut), jnp.float32),
            pltpu.SemaphoreType.DMA((3, SLOTS)),
        ],
        compiler_params=pltpu.CompilerParams(vmem_limit_bytes=48 * 2**20),
        name="project",
    )(live, start, high, low, left, right)


def local(devices, left_factor, right_factor, tile_counts, start_basis):
    high, low = sum_over_devices(tile_counts, left_factor, right_factor, devices)
    return project(left_factor, right_factor, tile_counts, start_basis, high, low)


def solution(mesh):
    return jax.shard_map(
        functools.partial(local, mesh.shape["rows"]),
        mesh=mesh,
        in_specs=(P("rows", None), P("rows", None), P("rows"), P()),
        out_specs=(P("rows", None), P("rows", None)),
        check_vma=False,
    )
```
